16 devices in a mesh: rep: 4 (over y, z, core), pp: 4 (over x).
Axes of the slice: x: 4, y: 2, z: 1, core: 2. Of those that a mesh axis runs over, the one named last changes fastest.
The devices are a block of a 4x4x8 slice.
Arguments:
- x: bfloat16 [32, 512, 640], P('rep'), parts along dimension 0
- dy: bfloat16 [32, 512, 640], P('rep'), parts along dimension 0
- w_gate: bfloat16 [4, 640, 1536], P('pp')
- w_up: bfloat16 [4, 640, 1536], P('pp')
- w_down: bfloat16 [4, 1536, 640], P('pp')
Outputs:
- output 1: bfloat16 [16, 640, 1536], P(('rep', 'pp')), parts along dimension 0
- output 2: bfloat16 [16, 640, 1536], P(('rep', 'pp')), parts along dimension 0
- output 3: bfloat16 [16, 1536, 640], P(('rep', 'pp')), parts along dimension 0
There are 4 independent parts. The reference program is written for one: setup_inputs(seed, part) draws one part's arguments, and reference() takes and returns one part's arrays. A program takes and returns all parts, laid end to end along the dimension named above; an argument that names none is the same for every part.
All inputs are finite; a program needn't handle non-finite values.
Results may differ from the reference program's by a relative error of at most 0.018.
Values are sent between devices in bfloat16 or wider.
A program may use at most 768 MiB of HBM per device.

```python
import jax
import jax.numpy as jnp
from jax import lax

MICRO = 8
TOKENS = 512
D = 640
FF = 1536
LAYERS = 4
NAMES = ("w_gate", "w_up", "w_down")
SHAPES = {"w_gate": (LAYERS, D, FF), "w_up": (LAYERS, D, FF), "w_down": (LAYERS, FF, D)}


def bump(key, n, height):
    away = (jnp.arange(n, dtype=jnp.int32) - jax.random.randint(key, (), 0, n, jnp.int32)) % n
    return jnp.where(away < n // 8, height, 1.0)


def together(key, own, strength):
    shared = jax.random.normal(key, own.shape[1:], jnp.float32)
    return (own + strength * shared) * lax.rsqrt(1 + strength * strength)


def setup_inputs(seed: int = 0, part: int = 0) -> dict:
    kx, kdy, ka, kb, kz, kf, kh, kl, *kw = jax.random.split(jax.random.key(seed), 8 + len(NAMES))
    kx, kdy, ka, kb = (jax.random.fold_in(k, part) for k in (kx, kdy, ka, kb))
    shape = (MICRO, TOKENS, D)
    much_x, much_dy = jax.random.uniform(kz, (2,), jnp.float32, 0.0, 1.0)
    layers = 2.0 ** jax.random.uniform(kl, (LAYERS, 1, 1), jnp.float32, -1.0, 1.0)
    x = together(ka, jax.random.normal(kx, shape, jnp.float32), much_x) * bump(kf, D, 4.0)
    dy = together(kb, jax.random.normal(kdy, shape, jnp.float32), much_dy)
    drawn = {"x": x.astype(jnp.bfloat16), "dy": (dy * (MICRO * TOKENS) ** -0.5).astype(jnp.bfloat16)}
    for key, name in zip(kw, NAMES, strict=True):
        w = jax.random.normal(key, SHAPES[name], jnp.float32) * SHAPES[name][1] ** -0.5
        drawn[name] = (w * {"w_gate": 1.0, "w_up": bump(kh, FF, 4.0), "w_down": layers}[name]).astype(jnp.bfloat16)
    return drawn


def matmul(a, w):
    return jnp.dot(a, w, preferred_element_type=jnp.float32).astype(jnp.bfloat16)


def normed(h):
    wide = h.astype(jnp.float32)
    scale = lax.rsqrt(jnp.mean(wide**2, -1, keepdims=True) + 1e-6)
    return (wide * scale).astype(jnp.bfloat16)


def layer(h, w):
    a = normed(h)
    gate = jnp.dot(a, w["w_gate"], preferred_element_type=jnp.float32)
    up = jnp.dot(a, w["w_up"], preferred_element_type=jnp.float32)
    return h + matmul((jax.nn.silu(gate) * up).astype(jnp.bfloat16), w["w_down"])


def stack(weights, h):
    return lax.scan(lambda h, w: (layer(h, w), None), h, weights)[0]


def reference(x, dy, w_gate, w_up, w_down):
    weights = dict(zip(NAMES, (w_gate, w_up, w_down), strict=True))

    def take(so_far, one):
        h, by_y = one
        _, back = jax.vjp(lambda w: stack(w, h), weights)
        return jax.tree.map(lambda total, term: total + term.astype(jnp.float32), so_far, back(by_y)[0]), None

    none_yet = {name: jnp.zeros(w.shape, jnp.float32) for name, w in weights.items()}
    by_weights, _ = lax.scan(take, none_yet, (x, dy))
    return tuple(by_weights[name].astype(jnp.bfloat16) for name in NAMES)
```

```python
import functools

import jax
import jax.numpy as jnp
from jax import lax
from jax.experimental import pallas as pl
from jax.experimental.pallas import tpu as pltpu
from jax.sharding import PartitionSpec as P

MESH = pl.DeviceIdType.MESH
CHUNK = 128
BLOCK = 512
LAG = 4
SLOTS = 4

f32, bf16 = jnp.float32, jnp.bfloat16


def dot(a, b):
    return jnp.dot(a, b, preferred_element_type=f32)


def norm_of(h):
    wide = h.astype(f32)
    return wide, lax.rsqrt(jnp.mean(wide * wide, -1, keepdims=True) + 1e-6)


def kernel(stages, micro, tokens, x, dy, wg_in, wu_in, wd_in, og, ou, od, wg, wu, wd, wgt, wut, wdt, sum_g, sum_u, sum_d, h_in, g_in,
           h_out, g_out, kept_g, kept_u, mid, act, dgate, dup, at, load_sem, h_recv, g_recv, h_send, g_send):
    me = lax.axis_index("pp")
    c, per = CHUNK, tokens // CHUNK
    chunks = micro * per
    ff, d = wd.shape
    ring = kept_g.shape[0]
    lag = (stages - 1 - me) * LAG
    first, last = me == 0, me == stages - 1

    loads = [pltpu.make_async_copy(src, dst, load_sem.at[n]) for n, (src, dst) in enumerate(((wg_in, wg), (wu_in, wu), (wd_in, wd)))]
    for load in loads:
        load.start()

    def rows(i):
        return pl.ds(pl.multiple_of(i * c, c), c)

    def fetch(src, dst, sem):
        def one(i, carry):
            pltpu.make_async_copy(src.at[rows(i), :], dst.at[rows(i), :], sem.at[i]).start()
            return carry
        lax.fori_loop(0, chunks, one, 0)

    @pl.when(first)
    def _():
        fetch(x, h_in, h_recv)

    @pl.when(last)
    def _():
        fetch(dy, g_in, g_recv)

    barrier = pltpu.get_barrier_semaphore()

    @pl.when(me > 0)
    def _():
        pl.semaphore_signal(barrier, inc=1, device_id={"pp": me - 1}, device_id_type=MESH)

    @pl.when(me < stages - 1)
    def _():
        pl.semaphore_signal(barrier, inc=1, device_id={"pp": me + 1}, device_id_type=MESH)

    pl.semaphore_wait(barrier, (me > 0).astype(jnp.int32) + (me < stages - 1).astype(jnp.int32))
    for load in loads:
        load.wait()

    def transposes():
        for n in range(0, ff, 256):
            s = slice(n, n + 256)
            wgt[s, :] = wg[:, s].T
            wut[s, :] = wu[:, s].T
            wdt[:, s] = wd[s, :].T

    def h_copy(i):
        return pltpu.make_async_remote_copy(
            src_ref=h_out.at[lax.rem(i, SLOTS)], dst_ref=h_in.at[rows(i), :], send_sem=h_send.at[lax.rem(i, SLOTS)], recv_sem=h_recv.at[i],
            device_id={"pp": me + 1}, device_id_type=MESH)

    def g_copy(i):
        return pltpu.make_async_remote_copy(
            src_ref=g_out.at[lax.rem(i, SLOTS)], dst_ref=g_in.at[rows(i), :], send_sem=g_send.at[lax.rem(i, SLOTS)], recv_sem=g_recv.at[i],
            device_id={"pp": me - 1}, device_id_type=MESH)

    def forward(i):
        pltpu.make_async_copy(h_in.at[rows(i), :], h_in.at[rows(i), :], h_recv.at[i]).wait()
        wide, scale = norm_of(h_in[rows(i), :])
        a = (wide * scale).astype(bf16)
        slot = lax.rem(i, ring)
        for n in range(0, ff, BLOCK):
            s = slice(n, n + BLOCK)
            gate, up = dot(a, wg[:, s]), dot(a, wu[:, s])
            kept_g[slot, :, s] = gate
            kept_u[slot, :, s] = up
            mid[:, s] = (gate * jax.nn.sigmoid(gate) * up).astype(bf16)

        @pl.when(me < stages - 1)
        def _():
            @pl.when(i >= SLOTS)
            def _():
                h_copy(i - SLOTS).wait_send()

            m = dot(mid[...], wd[...]).astype(bf16)
            h_out[lax.rem(i, SLOTS)] = (h_in[rows(i), :].astype(f32) + m.astype(f32)).astype(bf16)
            h_copy(i).start()

    def backward(i):
        pltpu.make_async_copy(g_in.at[rows(i), :], g_in.at[rows(i), :], g_recv.at[i]).wait()
        slot = lax.rem(i, ring)
        place = lax.rem(i, 2 * per)
        here = pl.ds(pl.multiple_of(place * c, c), c)

        @pl.when(first)
        def _():
            wide, scale = norm_of(h_in[rows(i), :])
            a = (wide * scale).astype(bf16)
            for n in range(0, ff, BLOCK):
                s = slice(n, n + BLOCK)
                kept_g[slot, :, s] = dot(a, wg[:, s])
                kept_u[slot, :, s] = dot(a, wu[:, s])

        g = g_in[rows(i), :]
        for n in range(0, ff, BLOCK):
            s = slice(n, n + BLOCK)
            by_act = dot(g, wdt[:, s]).astype(bf16).astype(f32)
            gate, up = kept_g[slot, :, s], kept_u[slot, :, s]
            part = jax.nn.sigmoid(gate)
            silu = gate * part
            act[here, s] = (silu * up).astype(bf16)
            dup[here, s] = (by_act * silu).astype(bf16)
            dgate[here, s] = (by_act * up * (part + silu * (1.0 - part))).astype(bf16)

        @pl.when(me > 0)
        def _():
            @pl.when(i >= SLOTS)
            def _():
                g_copy(i - SLOTS).wait_send()

            by_a = dot(dgate[here, :], wgt[...]).astype(bf16).astype(f32) + dot(dup[here, :], wut[...]).astype(bf16).astype(f32)
            by_a = by_a.astype(bf16).astype(f32)
            wide, scale = norm_of(h_in[rows(i), :])
            by_scale = jnp.sum(by_a * wide, -1, keepdims=True)
            by_h = by_a * scale - wide * (by_scale * scale * scale * scale * (1.0 / d))
            g_out[lax.rem(i, SLOTS)] = (g_in[rows(i), :].astype(f32) + by_h.astype(bf16).astype(f32)).astype(bf16)
            g_copy(i).start()

    def weights(m, q):
        half = pl.ds(pl.multiple_of(lax.rem(m, 2) * tokens, tokens), tokens)
        whole = pl.ds(pl.multiple_of(m * tokens, tokens), tokens)

        @pl.when(q == 0)
        def _():
            wide, scale = norm_of(h_in[whole, :])
            at[...] = (wide * scale).astype(bf16).T

        def add(total, here, s, left, right):
            term = dot(left, right).astype(bf16).astype(f32)
            total[here, s] = jnp.where(m == 0, 0.0, total[here, s]) + term

        part = d // per
        here = pl.ds(pl.multiple_of(q * part, part), part)
        left = at[here, :]
        for n in range(0, ff, BLOCK):
            s = slice(n, n + BLOCK)
            add(sum_g, here, s, left, dgate[half, s])
            add(sum_u, here, s, left, dup[half, s])
        part = ff // per
        here = pl.ds(pl.multiple_of(q * part, part), part)
        left = act[half, here].T
        add(sum_d, here, slice(None), left, g_in[whole, :])

    def step(t, carry):
        @pl.when(t < chunks)
        def _():
            forward(t)

        @pl.when(t == jnp.where(first, SLOTS - 1, 0))
        def _():
            transposes()

        j = t - lag

        @pl.when((j >= 0) & (j < chunks))
        def _():
            backward(j)

        @pl.when(j >= per)
        def _():
            weights(j // per - 1, lax.rem(j, per))
        return carry

    lax.fori_loop(0, lag + chunks + per, step, 0)

    for i in range(chunks - SLOTS, chunks):
        @pl.when(me < stages - 1)
        def _():
            h_copy(i).wait_send()

        @pl.when(me > 0)
        def _():
            g_copy(i).wait_send()

    stores = []
    for n, (total, staged, out) in enumerate(((sum_g, dgate.at[pl.ds(0, d), :], og), (sum_u, dup.at[pl.ds(0, d), :], ou), (sum_d, h_in.at[pl.ds(0, ff), :], od))):
        staged[...] = total[...].astype(bf16)
        stores.append(pltpu.make_async_copy(staged, out, load_sem.at[n]))
        stores[-1].start()
    for store in stores:
        store.wait()


def solution(mesh):
    stages = mesh.shape["pp"]

    def step(x, dy, w_gate, w_up, w_down):
        micro, tokens, d = x.shape
        ff = w_gate.shape[-1]
        chunks = micro * tokens // CHUNK
        ring = (stages - 2) * LAG + 1
        hbm = pl.BlockSpec(memory_space=pl.ANY)
        dma = pltpu.SemaphoreType.DMA
        outs = pl.pallas_call(
            functools.partial(kernel, stages, micro, tokens),
            out_shape=[jax.ShapeDtypeStruct(w.shape[1:], bf16) for w in (w_gate, w_up, w_down)],
            in_specs=[hbm] * 5,
            out_specs=[hbm] * 3,
            scratch_shapes=[
                pltpu.VMEM((d, ff), bf16), pltpu.VMEM((d, ff), bf16), pltpu.VMEM((ff, d), bf16),
                pltpu.VMEM((ff, d), bf16), pltpu.VMEM((ff, d), bf16), pltpu.VMEM((d, ff), bf16),
                pltpu.VMEM((d, ff), f32), pltpu.VMEM((d, ff), f32), pltpu.VMEM((ff, d), f32),
                pltpu.VMEM((micro * tokens, d), bf16), pltpu.VMEM((micro * tokens, d), bf16),
                pltpu.VMEM((SLOTS, CHUNK, d), bf16), pltpu.VMEM((SLOTS, CHUNK, d), bf16),
                pltpu.VMEM((ring, CHUNK, ff), f32), pltpu.VMEM((ring, CHUNK, ff), f32),
                pltpu.VMEM((CHUNK, ff), bf16),
                pltpu.VMEM((2 * tokens, ff), bf16), pltpu.VMEM((2 * tokens, ff), bf16), pltpu.VMEM((2 * tokens, ff), bf16),
                pltpu.VMEM((d, tokens), bf16),
                dma((3,)), dma((chunks,)), dma((chunks,)), dma((SLOTS,)), dma((SLOTS,)),
            ],
            compiler_params=pltpu.CompilerParams(collective_id=0, has_side_effects=True, vmem_limit_bytes=67043328),
        )(x.reshape(micro * tokens, d), dy.reshape(micro * tokens, d), w_gate[0], w_up[0], w_down[0])
        return tuple(out[None] for out in outs)

    return jax.shard_map(
        step,
        mesh=mesh,
        in_specs=(P("rep", None, None),) * 2 + (P("pp", None, None),) * 3,
        out_specs=(P(("rep", "pp"), None, None),) * 3,
        check_vma=False,
    )
```

```python
import functools

import jax
import jax.numpy as jnp
from jax import lax
from jax.experimental import pallas as pl
from jax.experimental.pallas import tpu as pltpu
from jax.sharding import PartitionSpec as P

MESH = pl.DeviceIdType.MESH
CHUNK = 128
BLOCK = 512
LAG = 4
SLOTS = 4

f32, bf16 = jnp.float32, jnp.bfloat16


def dot(a, b):
    return jnp.dot(a, b, preferred_element_type=f32)


def normed(h):
    wide = h.astype(f32)
    scale = lax.rsqrt(jnp.mean(wide * wide, -1, keepdims=True) + 1e-6)
    return wide, scale, (wide * scale).astype(bf16)


def kernel(stages, micro, tokens, x, dy, wg_in, wu_in, wd_in, sum_g, sum_u, sum_d, wg, wu, wd, wgt, wut, wdt, h_in, g_in,
           h_out, g_out, kept_g, kept_u, mid, act, dgate, dup, at, load_sem, h_recv, g_recv, h_send, g_send):
    me = lax.axis_index("pp")
    c, per = CHUNK, tokens // CHUNK
    chunks = micro * per
    ff, d = wd.shape
    ring = kept_g.shape[0]
    columns = [slice(n, n + BLOCK) for n in range(0, ff, BLOCK)]

    loads = [pltpu.make_async_copy(src, dst, load_sem.at[n]) for n, (src, dst) in enumerate(((wg_in, wg), (wu_in, wu), (wd_in, wd)))]
    for load in loads:
        load.start()

    def rows(i):
        return pl.ds(pl.multiple_of(i * c, c), c)

    def fetch(src, dst, sem):
        def one(i, carry):
            pltpu.make_async_copy(src.at[rows(i), :], dst.at[rows(i), :], sem.at[i]).start()
            return carry
        lax.fori_loop(0, chunks, one, 0)

    @pl.when(me == 0)
    def _():
        fetch(x, h_in, h_recv)

    @pl.when(me == stages - 1)
    def _():
        fetch(dy, g_in, g_recv)

    barrier = pltpu.get_barrier_semaphore()

    @pl.when(me > 0)
    def _():
        pl.semaphore_signal(barrier, inc=1, device_id={"pp": me - 1}, device_id_type=MESH)

    @pl.when(me < stages - 1)
    def _():
        pl.semaphore_signal(barrier, inc=1, device_id={"pp": me + 1}, device_id_type=MESH)

    pl.semaphore_wait(barrier, (me > 0).astype(jnp.int32) + (me < stages - 1).astype(jnp.int32))
    for load in loads:
        load.wait()

    def transposes():
        for n in range(0, ff, 256):
            s = slice(n, n + 256)
            wgt[s, :] = wg[:, s].T
            wut[s, :] = wu[:, s].T
            wdt[:, s] = wd[s, :].T

    def h_copy(i):
        return pltpu.make_async_remote_copy(
            src_ref=h_out.at[lax.rem(i, SLOTS)], dst_ref=h_in.at[rows(i), :], send_sem=h_send.at[lax.rem(i, SLOTS)], recv_sem=h_recv.at[i],
            device_id={"pp": me + 1}, device_id_type=MESH)

    def g_copy(i):
        return pltpu.make_async_remote_copy(
            src_ref=g_out.at[lax.rem(i, SLOTS)], dst_ref=g_in.at[rows(i), :], send_sem=g_send.at[lax.rem(i, SLOTS)], recv_sem=g_recv.at[i],
            device_id={"pp": me - 1}, device_id_type=MESH)

    def h_wait(i):
        pltpu.make_async_copy(h_in.at[rows(i), :], h_in.at[rows(i), :], h_recv.at[i]).wait()

    def g_wait(i):
        pltpu.make_async_copy(g_in.at[rows(i), :], g_in.at[rows(i), :], g_recv.at[i]).wait()

    def pieces(i):
        m, q = i // per - 1, lax.rem(i, per)
        half = pl.ds(pl.multiple_of(lax.rem(m, 2) * tokens, tokens), tokens)
        side = lax.rem(m, 2)
        whole = pl.ds(pl.multiple_of(m * tokens, tokens), tokens)

        def add(total, here, s, left, right):
            term = dot(left, right).astype(bf16).astype(f32)
            total[here, s] = jnp.where(m == 0, 0.0, total[here, s]) + term

        share = d // per
        here = pl.ds(pl.multiple_of(q * share, share), share)

        def gate_up(total, by, s):
            add(total, here, s, at[side, here, :], by[half, s])

        def down(n, size):
            there = pl.ds(pl.multiple_of(q * (ff // per) + n, 128), size)
            add(sum_d, there, slice(None), act[half, there].T, g_in[whole, :])

        work = [functools.partial(gate_up, total, by, s) for total, by in ((sum_g, dgate), (sum_u, dup)) for s in columns]
        return work + [functools.partial(down, n, 128) for n in range(0, ff // per, 128)]

    def do(work):
        for piece in work:
            piece()

    def expand(i, a, s, slot):
        gate, up = dot(a, wg[:, s]), dot(a, wu[:, s])
        kept_g[slot, :, s] = gate
        kept_u[slot, :, s] = up
        return gate, up

    def forward(i, role, work):
        h_wait(i)

        @pl.when(i >= SLOTS)
        def _():
            h_copy(i - SLOTS).wait_send()

        do(work[:1])
        a = normed(h_in[rows(i), :])[2]
        for s in columns:
            gate, up = dot(a, wg[:, s]), dot(a, wu[:, s])
            if role == "middle":
                kept_g[lax.rem(i, ring), :, s] = gate
                kept_u[lax.rem(i, ring), :, s] = up
            mid[:, s] = (gate * jax.nn.sigmoid(gate) * up).astype(bf16)
        do(work[1:3])
        m = dot(mid[...], wd[...]).astype(bf16)
        do(work[3:])
        h_out[lax.rem(i, SLOTS)] = (h_in[rows(i), :].astype(f32) + m.astype(f32)).astype(bf16)
        h_copy(i).start()

    def backward(i, role, work):
        if role == "last":
            h_wait(i)
        g_wait(i)
        if role != "first":
            @pl.when(i >= SLOTS)
            def _():
                g_copy(i - SLOTS).wait_send()
        place = lax.rem(i, 2 * per)
        here = pl.ds(pl.multiple_of(place * c, c), c)
        do(work[:1])
        wide, scale, a = normed(h_in[rows(i), :])
        at[lax.rem(i // per, 2), :, pl.ds(pl.multiple_of(lax.rem(i, per) * c, c), c)] = a.T
        g = g_in[rows(i), :]
        for s in columns:
            if role == "middle":
                gate, up = kept_g[lax.rem(i, ring), :, s], kept_u[lax.rem(i, ring), :, s]
            else:
                gate, up = dot(a, wg[:, s]), dot(a, wu[:, s])
            by_act = dot(g, wdt[:, s]).astype(bf16).astype(f32)
            part = jax.nn.sigmoid(gate)
            silu = gate * part
            act[here, s] = (silu * up).astype(bf16)
            dup[here, s] = (by_act * silu).astype(bf16)
            dgate[here, s] = (by_act * up * (part + silu * (1.0 - part))).astype(bf16)
        if role == "first":
            do(work[1:])
            return
        do(work[1:3])
        by_a = dot(dgate[here, :], wgt[...]).astype(bf16).astype(f32) + dot(dup[here, :], wut[...]).astype(bf16).astype(f32)
        do(work[3:])
        by_a = by_a.astype(bf16).astype(f32)
        by_scale = jnp.sum(by_a * wide, -1, keepdims=True)
        by_h = by_a * scale - wide * (by_scale * scale * scale * scale * (1.0 / d))
        g_out[lax.rem(i, SLOTS)] = (g_in[rows(i), :].astype(f32) + by_h.astype(bf16).astype(f32)).astype(bf16)
        g_copy(i).start()

    def loop(start, stop, body):
        def one(t, carry):
            body(t)
            return carry
        lax.fori_loop(start, stop, one, 0)

    def run(role):
        lag = (stages - 1 - me) * LAG

        def step(t):
            i = t - lag
            steady = (t >= lag + per) & (t < chunks)

            @pl.when(steady)
            def _():
                work = pieces(i)
                if role == "last":
                    backward(i, role, [])
                    do(work)
                else:
                    forward(t, role, work[:4])
                    backward(i, role, work[4:])

            if role != "last":
                @pl.when((t < chunks) & ~steady)
                def _():
                    forward(t, role, [])

            if role == "first":
                pl.when(t == SLOTS - 1)(transposes)

            @pl.when((i >= 0) & (i < chunks) & ~steady)
            def _():
                backward(i, role, [])

            @pl.when((i >= per) & ~steady)
            def _():
                do(pieces(i))

        if role != "first":
            transposes()
        loop(0, lag + chunks + per, step)
        for i in range(chunks - SLOTS, chunks):
            if role != "last":
                h_copy(i).wait_send()
            if role != "first":
                g_copy(i).wait_send()

    @pl.when(me == 0)
    def _():
        run("first")

    @pl.when((me > 0) & (me < stages - 1))
    def _():
        run("middle")

    @pl.when(me == stages - 1)
    def _():
        run("last")


def finish(sum_g, sum_u, sum_d, og, ou, od, by_g, by_u, by_d, sem):
    stores = []
    for n, (total, staged, out) in enumerate(((sum_g, by_g, og), (sum_u, by_u, ou), (sum_d, by_d, od))):
        size = total.shape[0] // 4
        for part in range(4):
            here = pl.ds(part * size, size)
            staged[here, :] = total[here, :].astype(bf16)
            stores.append(pltpu.make_async_copy(staged.at[here, :], out.at[here, :], sem.at[n * 4 + part]))
            stores[-1].start()
    for store in stores:
        store.wait()


def solution(mesh):
    stages = mesh.shape["pp"]

    def step(x, dy, w_gate, w_up, w_down):
        micro, tokens, d = x.shape
        ff = w_gate.shape[-1]
        chunks = micro * tokens // CHUNK
        ring = (stages - 2) * LAG + 1
        hbm = pl.BlockSpec(memory_space=pl.ANY)
        dma = pltpu.SemaphoreType.DMA
        shapes = [w.shape[1:] for w in (w_gate, w_up, w_down)]
        sums = pl.pallas_call(
            functools.partial(kernel, stages, micro, tokens),
            out_shape=[pltpu.VMEM(shape, f32) for shape in shapes],
            in_specs=[hbm] * 5,
            out_specs=[pl.BlockSpec(memory_space=pltpu.VMEM)] * 3,
            scratch_shapes=[
                pltpu.VMEM((d, ff), bf16), pltpu.VMEM((d, ff), bf16), pltpu.VMEM((ff, d), bf16),
                pltpu.VMEM((ff, d), bf16), pltpu.VMEM((ff, d), bf16), pltpu.VMEM((d, ff), bf16),
                pltpu.VMEM((micro * tokens, d), bf16), pltpu.VMEM((micro * tokens, d), bf16),
                pltpu.VMEM((SLOTS, CHUNK, d), bf16), pltpu.VMEM((SLOTS, CHUNK, d), bf16),
                pltpu.VMEM((ring, CHUNK, ff), f32), pltpu.VMEM((ring, CHUNK, ff), f32),
                pltpu.VMEM((CHUNK, ff), bf16),
                pltpu.VMEM((2 * tokens, ff), bf16), pltpu.VMEM((2 * tokens, ff), bf16), pltpu.VMEM((2 * tokens, ff), bf16),
                pltpu.VMEM((2, d, tokens), bf16),
                dma((3,)), dma((chunks,)), dma((chunks,)), dma((SLOTS,)), dma((SLOTS,)),
            ],
            compiler_params=pltpu.CompilerParams(collective_id=0, has_side_effects=True, vmem_limit_bytes=50 * 2**20),
        )(x.reshape(micro * tokens, d), dy.reshape(micro * tokens, d), w_gate[0], w_up[0], w_down[0])
        outs = pl.pallas_call(
            finish,
            out_shape=[jax.ShapeDtypeStruct(shape, bf16) for shape in shapes],
            in_specs=[pl.BlockSpec(memory_space=pltpu.VMEM)] * 3,
            out_specs=[hbm] * 3,
            scratch_shapes=[pltpu.VMEM(shape, bf16) for shape in shapes] + [dma((12,))],
            compiler_params=pltpu.CompilerParams(vmem_limit_bytes=16 * 2**20),
        )(*sums)
        return tuple(out[None] for out in outs)

    return jax.shard_map(
        step,
        mesh=mesh,
        in_specs=(P("rep", None, None),) * 2 + (P("pp", None, None),) * 3,
        out_specs=(P(("rep", "pp"), None, None),) * 3,
        check_vma=False,
    )
```

```python
import functools

import jax
import jax.numpy as jnp
from jax import lax
from jax.experimental import pallas as pl
from jax.experimental.pallas import tpu as pltpu
from jax.sharding import PartitionSpec as P

MESH = pl.DeviceIdType.MESH
CHUNK = 128
BLOCK = 512
ENDS = 2
LAG = 4
SLOTS = 3

f32, bf16 = jnp.float32, jnp.bfloat16


def dot(a, b):
    return jnp.dot(a, b, preferred_element_type=f32)


def normed(h):
    wide = h.astype(f32)
    scale = lax.rsqrt(jnp.mean(wide * wide, -1, keepdims=True) + 1e-6)
    return wide, scale, (wide * scale).astype(bf16)


def kernel(stages, micro, tokens, x, dy, wg_in, wu_in, wd_in, sum_g, sum_u, sum_d, wg, wu, wd, wgt, wut, wdt, h_in, g_in,
           h_out, g_out, kept_g, kept_u, mid, act, dgate, dup, new_dgate, new_dup, at, load_sem, h_recv, g_recv, h_send, g_send):
    me = lax.axis_index("pp")
    c, per, small = CHUNK, tokens // CHUNK, CHUNK // ENDS
    chunks = micro * per
    items = chunks - 2 + 2 * ENDS
    tail = items - ENDS
    ff, d = wd.shape
    ring = kept_g.shape[0]
    new_by, new_act = mid.at[0], mid.at[1]
    columns = [slice(n, n + BLOCK) for n in range(0, ff, BLOCK)]

    def begin(i):
        return jnp.where(i < ENDS, i * small, jnp.where(i < tail, (i - ENDS + 1) * c, (chunks - 1) * c + (i - tail) * small))

    def rows(i, size):
        return pl.ds(pl.multiple_of(begin(i), small), size)

    def whole(i):
        return (i >= ENDS) & (i < tail)

    def fetch(src, dst, sem, since, until):
        for start, stop, size in ((0, ENDS, small), (ENDS, tail, c), (tail, items, small)):
            if not since <= start < until:
                continue

            def one(i, carry):
                pltpu.make_async_copy(src.at[rows(i, size), :], dst.at[rows(i, size), :], sem.at[i]).start()
                return carry
            lax.fori_loop(start, stop, one, 0)

    @pl.when(me == 0)
    def _():
        fetch(x, h_in, h_recv, 0, ENDS)

    @pl.when(me == stages - 1)
    def _():
        fetch(dy, g_in, g_recv, 0, ENDS)

    loads = [pltpu.make_async_copy(src, dst, load_sem.at[n]) for n, (src, dst) in enumerate(((wg_in, wg), (wu_in, wu), (wd_in, wd)))]
    for load in loads:
        load.start()

    @pl.when(me == 0)
    def _():
        fetch(x, h_in, h_recv, ENDS, items)

    @pl.when(me == stages - 1)
    def _():
        fetch(dy, g_in, g_recv, ENDS, items)

    barrier = pltpu.get_barrier_semaphore()

    @pl.when(me > 0)
    def _():
        pl.semaphore_signal(barrier, inc=1, device_id={"pp": me - 1}, device_id_type=MESH)

    @pl.when(me < stages - 1)
    def _():
        pl.semaphore_signal(barrier, inc=1, device_id={"pp": me + 1}, device_id_type=MESH)

    pl.semaphore_wait(barrier, (me > 0).astype(jnp.int32) + (me < stages - 1).astype(jnp.int32))
    for load in loads:
        load.wait()

    def prepare():
        for n in range(0, ff, 256):
            s = slice(n, n + 256)
            wgt[s, :] = wg[:, s].T
            wut[s, :] = wu[:, s].T
            wdt[:, s] = wd[s, :].T
        for total in (sum_g, sum_u, sum_d):
            total[...] = jnp.zeros_like(total)

    def h_copy(i, size):
        slot = lax.rem(i, SLOTS)
        return pltpu.make_async_remote_copy(
            src_ref=h_out.at[slot, pl.ds(0, size), :], dst_ref=h_in.at[rows(i, size), :], send_sem=h_send.at[slot], recv_sem=h_recv.at[i],
            device_id={"pp": me + 1}, device_id_type=MESH)

    def g_copy(i, size):
        slot = lax.rem(i, SLOTS)
        return pltpu.make_async_remote_copy(
            src_ref=g_out.at[slot, pl.ds(0, size), :], dst_ref=g_in.at[rows(i, size), :], send_sem=g_send.at[slot], recv_sem=g_recv.at[i],
            device_id={"pp": me - 1}, device_id_type=MESH)

    def sent(copy, i):
        @pl.when((i >= 0) & whole(i))
        def _():
            copy(i, c).wait_send()

        @pl.when((i >= 0) & ~whole(i))
        def _():
            copy(i, small).wait_send()

    def h_wait(i, size):
        pltpu.make_async_copy(h_in.at[rows(i, size), :], h_in.at[rows(i, size), :], h_recv.at[i]).wait()

    def g_wait(i, size):
        pltpu.make_async_copy(g_in.at[rows(i, size), :], g_in.at[rows(i, size), :], g_recv.at[i]).wait()

    def pieces(i):
        m, q = i // per - 1, lax.rem(i, per)
        half = pl.ds(pl.multiple_of(lax.rem(m, 2) * tokens, tokens), tokens)
        side = lax.rem(m, 2)
        batch = pl.ds(pl.multiple_of(m * tokens, tokens), tokens)

        def add(total, here, s, left, right):
            term = dot(left, right).astype(bf16).astype(f32)
            total[here, s] += term

        share = d // per
        here = pl.ds(pl.multiple_of(q * share, share), share)

        def gate_up(total, by, s):
            add(total, here, s, at[side, here, :], by[half, s])

        def down(n, size):
            there = pl.ds(pl.multiple_of(q * (ff // per) + n, 128), size)
            add(sum_d, there, slice(None), act[half, there].T, g_in[batch, :])

        work = [functools.partial(gate_up, total, by, s) for total, by in ((sum_g, dgate), (sum_u, dup)) for s in columns]
        return work + [functools.partial(down, n, 128) for n in range(0, ff // per, 128)]

    def do(work):
        for piece in work:
            piece()

    def expand(i, a, s, slot):
        gate, up = dot(a, wg[:, s]), dot(a, wu[:, s])
        kept_g[slot, :, s] = gate
        kept_u[slot, :, s] = up
        return gate, up

    def expand(a, s, out):
        gate, up = dot(a, wg[:, s]), dot(a, wu[:, s])
        part = jax.nn.sigmoid(gate)
        silu = gate * part
        out[:, s] = (silu * up).astype(bf16)
        return up * (part + silu * (1.0 - part)), silu

    def place(i, size):
        return pl.ds(pl.multiple_of(lax.rem(begin(i), 2 * tokens), size), size)

    def forward(i, size, role, head=(), tail=()):
        h_wait(i, size)
        sent(h_copy, i - SLOTS)
        slot = lax.rem(i, ring) if role == "middle" else 0
        do(head)
        a = normed(h_in[rows(i, size), :])[2]
        for s in columns:
            to_gate, to_up = expand(a, s, mid.at[slot, pl.ds(0, size), :])
            if role == "middle":
                kept_g[slot, :size, s] = to_gate
                kept_u[slot, :size, s] = to_up
        m = dot(mid[slot, :size, :], wd[...]).astype(bf16)
        do(tail)
        h_out[lax.rem(i, SLOTS), :size] = (h_in[rows(i, size), :].astype(f32) + m.astype(f32)).astype(bf16)
        h_copy(i, size).start()

    def keep(a, start):
        at[lax.rem(start // tokens, 2), :, pl.ds(pl.multiple_of(lax.rem(start, tokens), c), c)] = a.T

    def again(i, size):
        a = normed(h_in[rows(i, size), :])[2]
        for s in columns:
            kept_g[0, :size, s], kept_u[0, :size, s] = expand(a, s, new_act.at[pl.ds(0, size), :])
        if size == c:
            keep(a, begin(i))

    def backward(i, size, role, head=(), tail=()):
        here, slot = place(i, size), lax.rem(i, ring) if role == "middle" else 0
        if role == "middle":
            if size == c:
                keep(normed(h_in[rows(i, size), :])[2], begin(i))
            act[here, :] = mid[slot, :size, :]
        g_wait(i, size)
        if role != "first":
            sent(g_copy, i - SLOTS)
        if role == "last":
            new_by[:size, :] = dot(g_in[rows(i, size), :], wdt[...]).astype(bf16)
            h_wait(i, size)
        if role != "first":
            wide, scale, a = normed(h_in[rows(i, size), :])
        if role == "last" and size == c:
            keep(a, begin(i))

        def store():
            if role != "middle":
                act[here, :] = new_act[:size, :]
            dup[here, :] = new_dup[:size, :]
            dgate[here, :] = new_dgate[:size, :]

        g = g_in[rows(i, size), :]
        for s in columns:
            by_act = new_by[:size, s] if role == "last" else dot(g, wdt[:, s]).astype(bf16)
            by_act = by_act.astype(f32)
            if role == "last":
                to_gate, to_up = expand(a, s, new_act.at[pl.ds(0, size), :])
            else:
                to_gate, to_up = kept_g[slot, :size, s], kept_u[slot, :size, s]
            new_dup[:size, s] = (by_act * to_up).astype(bf16)
            new_dgate[:size, s] = (by_act * to_gate).astype(bf16)
        do(head)
        if role != "first":
            by_a = dot(new_dgate[:size, :], wgt[...]).astype(bf16).astype(f32) + dot(new_dup[:size, :], wut[...]).astype(bf16).astype(f32)
            do(tail)
            store()
            by_a = by_a.astype(bf16).astype(f32)
            by_scale = jnp.sum(by_a * wide, -1, keepdims=True)
            by_h = by_a * scale - wide * (by_scale * scale * scale * scale * (1.0 / d))
            g_out[lax.rem(i, SLOTS), :size] = (g_in[rows(i, size), :].astype(f32) + by_h.astype(bf16).astype(f32)).astype(bf16)
            g_copy(i, size).start()
        else:
            do(tail)
            store()
        if size != c:
            @pl.when((i == ENDS - 1) | (i == items - 1))
            def _():
                first = begin(i) - (ENDS - 1) * small
                keep(normed(h_in[pl.ds(pl.multiple_of(first, c), c), :])[2], first)

    def loop(start, stop, body):
        def one(t, carry):
            body(t)
            return carry
        lax.fori_loop(start, stop, one, 0)

    def run(role):
        lag = jnp.where(me < stages - 1, LAG * (stages - 1 - me) - 1, 0)

        def share(i):
            return jnp.where(i < items, i - ENDS + 1, i - items + chunks)

        def step(t):
            i = t - lag
            steady = whole(t) & (i >= per + ENDS - 1) & (i < tail)

            @pl.when(steady)
            def _():
                work = pieces(share(i))
                if role == "last":
                    backward(i, c, role)
                    do(work)
                elif role == "middle":
                    forward(t, c, role)
                    do(work)
                    backward(i, c, role)
                else:
                    forward(t, c, role, work[:1], [functools.partial(again, i, c)] + work[1:2])
                    backward(i, c, role, work[2:4], work[4:])

            @pl.when(~steady)
            def _():
                for size, right in ((c, whole), (small, lambda i: ~whole(i))):
                    if role != "last":
                        @pl.when((t < items) & right(t))
                        def _():
                            forward(t, size, role)

                if role == "first":
                    pl.when(t == ENDS + 1)(prepare)

                for size, right in ((c, whole), (small, lambda i: ~whole(i))):
                    @pl.when((i >= 0) & (i < items) & right(i))
                    def _():
                        if role == "first":
                            again(i, size)
                        backward(i, size, role)

                @pl.when((i >= per + ENDS - 1) & (i <= tail) | (i >= items))
                def _():
                    do(pieces(share(i)))

        if role != "first":
            prepare()
        loop(0, lag + items + per, step)
        for i in range(items - SLOTS, items):
            if role != "last":
                sent(h_copy, i)
            if role != "first":
                sent(g_copy, i)

    @pl.when(me == 0)
    def _():
        run("first")

    @pl.when((me > 0) & (me < stages - 1))
    def _():
        run("middle")

    @pl.when(me == stages - 1)
    def _():
        run("last")


def finish(sum_g, sum_u, sum_d, og, ou, od, by_g, by_u, by_d, sem):
    stores = []
    for n, (total, staged, out) in enumerate(((sum_g, by_g, og), (sum_u, by_u, ou), (sum_d, by_d, od))):
        size = total.shape[0] // 4
        for part in range(4):
            here = pl.ds(part * size, size)
            staged[here, :] = total[here, :].astype(bf16)
            stores.append(pltpu.make_async_copy(staged.at[here, :], out.at[here, :], sem.at[n * 4 + part]))
            stores[-1].start()
    for store in stores:
        store.wait()


def solution(mesh):
    stages = mesh.shape["pp"]

    def step(x, dy, w_gate, w_up, w_down):
        micro, tokens, d = x.shape
        ff = w_gate.shape[-1]
        items = micro * tokens // CHUNK - 2 + 2 * ENDS
        ring = (stages - 2) * LAG
        hbm = pl.BlockSpec(memory_space=pl.ANY)
        dma = pltpu.SemaphoreType.DMA
        shapes = [w.shape[1:] for w in (w_gate, w_up, w_down)]
        sums = pl.pallas_call(
            functools.partial(kernel, stages, micro, tokens),
            out_shape=[pltpu.VMEM(shape, f32) for shape in shapes],
            in_specs=[hbm] * 5,
            out_specs=[pl.BlockSpec(memory_space=pltpu.VMEM)] * 3,
            scratch_shapes=[
                pltpu.VMEM((d, ff), bf16), pltpu.VMEM((d, ff), bf16), pltpu.VMEM((ff, d), bf16),
                pltpu.VMEM((ff, d), bf16), pltpu.VMEM((ff, d), bf16), pltpu.VMEM((d, ff), bf16),
                pltpu.VMEM((micro * tokens, d), bf16), pltpu.VMEM((micro * tokens, d), bf16),
                pltpu.VMEM((SLOTS, CHUNK, d), bf16), pltpu.VMEM((SLOTS, CHUNK, d), bf16),
                pltpu.VMEM((ring, CHUNK, ff), f32), pltpu.VMEM((ring, CHUNK, ff), f32),
                pltpu.VMEM((ring, CHUNK, ff), bf16),
                pltpu.VMEM((2 * tokens, ff), bf16), pltpu.VMEM((2 * tokens, ff), bf16), pltpu.VMEM((2 * tokens, ff), bf16),
                pltpu.VMEM((CHUNK, ff), bf16), pltpu.VMEM((CHUNK, ff), bf16),
                pltpu.VMEM((2, d, tokens), bf16),
                dma((3,)), dma((items,)), dma((items,)), dma((SLOTS,)), dma((SLOTS,)),
            ],
            compiler_params=pltpu.CompilerParams(collective_id=0, has_side_effects=True, vmem_limit_bytes=int(52.5 * 2**20)),
        )(x.reshape(micro * tokens, d), dy.reshape(micro * tokens, d), w_gate[0], w_up[0], w_down[0])
        outs = pl.pallas_call(
            finish,
            out_shape=[jax.ShapeDtypeStruct(shape, bf16) for shape in shapes],
            in_specs=[pl.BlockSpec(memory_space=pltpu.VMEM)] * 3,
            out_specs=[hbm] * 3,
            scratch_shapes=[pltpu.VMEM(shape, bf16) for shape in shapes] + [dma((12,))],
            compiler_params=pltpu.CompilerParams(vmem_limit_bytes=16 * 2**20),
        )(*sums)
        return tuple(out[None] for out in outs)

    return jax.shard_map(
        step,
        mesh=mesh,
        in_specs=(P("rep", None, None),) * 2 + (P("pp", None, None),) * 3,
        out_specs=(P(("rep", "pp"), None, None),) * 3,
        check_vma=False,
    )
```
